32 devices in a mesh: dp: 16 (over z, y, x), tensor: 2 (over core).
Axes of the slice: x: 2, y: 2, z: 4, core: 2. Of those that a mesh axis runs over, the one named last changes fastest.
Arguments:
- hidden: bfloat16 [16384, 7168], P('dp', 'tensor'), parts along dimension 0, may hold values from -6 to 6
- w_dq: bfloat16 [7168, 1536], P('tensor'), may hold values from -0.0625 to 0.0625
- w_dkv: bfloat16 [7168, 576], P('tensor'), may hold values from -0.0625 to 0.0625
- q_gain: float32 [1536], replicated, may hold values from 0.1 to 1.9
- kv_gain: float32 [512], replicated, may hold values from 0.1 to 1.9
- w_uq: bfloat16 [1536, 12288], P(None, 'tensor'), may hold values from -0.15625 to 0.15625
- w_ukv: bfloat16 [512, 16384], P(None, 'tensor'), may hold values from -0.25 to 0.25
Outputs:
- queries: bfloat16 [16384, 12288], P('dp', 'tensor'), parts along dimension 0
- keys_values: bfloat16 [16384, 16384], P('dp', 'tensor'), parts along dimension 0
- rotary_key: bfloat16 [16384, 64], P(('dp', 'tensor')), parts along dimension 0
The draws below stay inside these ranges and needn't reach their ends.
There are 16 independent parts, one for each index of `dp`. The reference program is written for one: setup_inputs(seed, part) draws one part's arguments, and reference() takes and returns one part's arrays. A program takes and returns all parts, laid end to end along the dimension named above; an argument that names none is the same for every part. Nothing has to cross between parts.
All inputs are finite; a program needn't handle non-finite values.
Results may differ from the reference program's by a relative error of at most 0.0049.
Values may be sent and summed in bfloat16 or wider, within the bound.
A program may use at most 192 MiB of HBM per device.

```python
import jax
import jax.numpy as jnp
from jax import lax

D = 7168
QL = 1536
KL = 512
HEADS = 64
NOPE = 128
ROPE = 64
VDIM = 128
TOK = 1024


def block_scale(own_key, shape, split, least, top_value):
    level = 1.0
    for dim, shards_of in split:
        draws = jax.random.uniform(jax.random.fold_in(jax.random.fold_in(own_key, 6), dim), (shards_of,), jnp.float32, least / len(split), top_value / len(split))
        level = level * jnp.repeat(jnp.exp(draws), shape[dim] // shards_of).reshape((-1,) + (1,) * (len(shape) - 1 - dim))
    return level


def scatter_about(rng, dims, spread, most, shards=(), kind=jnp.bfloat16):
    result = jax.random.normal(rng, dims, jnp.float32) * spread
    if len(shards) > 0:
        result = block_scale(rng, dims, shards, -0.22, 0.18) * result
    return jnp.clip(result, min=-most, max=most).astype(kind)


def setup_inputs(seed: int = 0, part: int = 0) -> dict:
    seeds = jax.random.split(jax.random.key(seed), 8)
    part_keys = jax.random.split(jax.random.fold_in(seeds[7], part), 8)
    hidden = scatter_about(part_keys[0], (TOK, D), 1.0, 6.0, ((1, 2),))
    w_dq = scatter_about(seeds[1], (D, QL), D ** -0.5, 0.0625, ((0, 2),))
    w_dkv = scatter_about(seeds[2], (D, KL + ROPE), D ** -0.5, 0.0625, ((0, 2),))
    q_gain = jnp.clip(1.0 + 0.18 * jax.random.normal(seeds[3], (QL,), jnp.float32), 0.1, 1.9)
    kv_gain = jnp.clip(1.0 + 0.18 * jax.random.normal(seeds[4], (KL,), jnp.float32), 0.1, 1.9)
    w_uq = scatter_about(seeds[5], (QL, HEADS * (NOPE + ROPE)), QL ** -0.5, 0.15625, ((1, 2),))
    w_ukv = scatter_about(seeds[6], (KL, HEADS * (NOPE + VDIM)), KL ** -0.5, 0.25, ((1, 2),))
    return dict(hidden=hidden, w_dq=w_dq, w_dkv=w_dkv, q_gain=q_gain, kv_gain=kv_gain, w_uq=w_uq, w_ukv=w_ukv)


def rotate(values, angle):
    half = values.shape[-1] // 2
    first = values[..., :half]
    second = values[..., half:]
    cosine = jnp.cos(angle)
    sine = jnp.sin(angle)
    return jnp.concatenate([first * cosine - second * sine, second * cosine + first * sine], axis=-1)

def angles(positions, half):
    freqs = 50000.0 ** (-jnp.arange(half, dtype=jnp.float32) / half)
    return positions[:, None] * freqs[None, :]

def normalize(block, gain):
    scale = lax.rsqrt(lax.optimization_barrier(jnp.mean(block * block, axis=1, keepdims=True)) + 1e-06)
    return (block * scale * gain[None, :]).astype(jnp.bfloat16)

def reference(hidden, w_dq, w_dkv, q_gain, kv_gain, w_uq, w_ukv):
    down = jnp.concatenate([jnp.dot(hidden, w_dq, preferred_element_type=jnp.float32), jnp.dot(hidden, w_dkv, preferred_element_type=jnp.float32)], axis=1)
    q_latent = normalize(down[:, :QL], q_gain)
    kv_latent = normalize(down[:, QL:QL + KL], kv_gain)
    positions = jnp.arange(TOK, dtype=jnp.float32)
    angle = angles(positions, ROPE // 2)
    rotary_key = rotate(down[:, QL + KL:], angle).astype(jnp.bfloat16)
    query_full = jnp.dot(q_latent, w_uq, preferred_element_type=jnp.float32)
    query_full = query_full.reshape(TOK, HEADS, NOPE + ROPE)
    turned = rotate(query_full[:, :, NOPE:], angle[:, None, :])
    queries = jnp.concatenate([query_full[:, :, :NOPE], turned], axis=2)
    queries = queries.reshape(TOK, HEADS * (NOPE + ROPE)).astype(jnp.bfloat16)
    keys_values = jnp.dot(kv_latent, w_ukv, preferred_element_type=jnp.float32).astype(jnp.bfloat16)
    return (queries, keys_values, rotary_key)
```

```python
import functools

import jax
import jax.numpy as jnp
import numpy as np
from jax import lax
from jax.experimental import pallas as pl
from jax.experimental.pallas import tpu as pltpu
from jax.sharding import PartitionSpec as P

NOPE = 128
ROPE = 64
CHUNKS = 4
HEADS_PER_STEP = 4
F32 = jnp.float32
BF16 = jnp.bfloat16


def table(count, half):
    freqs = np.float32(50000.0) ** (-np.arange(half, dtype=np.float32) / np.float32(half))
    angle = np.arange(count, dtype=np.float32)[:, None] * freqs.astype(np.float32)[None, :]
    angle = angle.astype(np.float64)
    both = np.concatenate([np.cos(angle), np.sin(angle)], axis=1).astype(np.float32)
    return np.concatenate([both, both], axis=1)


def down_kernel(
    hidden_hbm, w_dq_hbm, w_dkv_t_hbm, q_gain, kv_gain,
    q_lat, kv_lat, key_sum,
    hidden, w_q, w_kv, acc, key_acc, send, recv, key_send, key_recv,
    hid_sem, w_sem, send_sem, recv_sem,
):
    me = lax.axis_index("tensor")
    other = 1 - me
    rows = hidden.shape[0]
    width = acc.shape[2]
    q_blocks = w_q.shape[0]
    blocks = q_blocks + 1
    part = rows // CHUNKS
    share = key_recv.shape[1]
    across = (((1,), (1,)), ((), ()))

    def load_hidden(m):
        at = pl.ds(m * part, part)
        return pltpu.make_async_copy(hidden_hbm.at[at], hidden.at[at], hid_sem.at[m])

    def load_w(n):
        if n < q_blocks:
            return pltpu.make_async_copy(
                w_dq_hbm.at[:, pl.ds(n * width, width)], w_q.at[n], w_sem.at[n]
            )
        return pltpu.make_async_copy(w_dkv_t_hbm, w_kv, w_sem.at[n])

    def exchange(n):
        return pltpu.make_async_remote_copy(
            src_ref=send.at[n], dst_ref=recv.at[n],
            send_sem=send_sem.at[n], recv_sem=recv_sem.at[n],
            device_id={"tensor": other}, device_id_type=pl.DeviceIdType.MESH,
        )

    load_hidden(0).start()
    load_w(0).start()
    for m in range(1, CHUNKS):
        load_hidden(m).start()
    for n in range(1, blocks):
        load_w(n).start()

    barrier = pltpu.get_barrier_semaphore()
    pl.semaphore_signal(
        barrier, inc=1, device_id={"tensor": other}, device_id_type=pl.DeviceIdType.MESH
    )
    pl.semaphore_wait(barrier, 1)

    def gather(n):
        total = acc[n] + recv[n].astype(F32)
        acc[n] = total
        return jnp.sum(total * total, axis=1, keepdims=True)

    load_w(0).wait()
    for m in range(CHUNKS):
        load_hidden(m).wait()
        at = pl.ds(m * part, part)
        piece = jnp.dot(hidden[at], w_q[0], preferred_element_type=F32)
        acc[0, at] = piece
        send[0, at] = piece.astype(BF16)
    exchange(0).start()

    squares = None
    for n in range(1, blocks):
        load_w(n).wait()
        if n >= 2:
            exchange(n - 2).wait_recv()
        if n < q_blocks:
            piece = jnp.dot(hidden[...], w_q[n], preferred_element_type=F32)
        else:
            piece = lax.dot_general(
                hidden[...], w_kv[:width], across, preferred_element_type=F32
            )
        acc[n] = piece
        send[n] = piece.astype(BF16)
        if n >= 2:
            more = gather(n - 2)
            squares = more if squares is None else squares + more
        exchange(n).start()

    exchange(q_blocks - 1).wait_recv()
    piece = lax.dot_general(
        w_kv[width:], hidden[...], across, preferred_element_type=F32
    )
    key_acc[...] = piece
    key_send[...] = piece.astype(BF16)
    more = gather(q_blocks - 1)
    squares = more if squares is None else squares + more
    scale = lax.rsqrt(squares / (q_blocks * width) + 1e-06)
    for n in range(q_blocks):
        at = pl.ds(n * width, width)
        q_lat[:, at] = (acc[n] * scale * q_gain[at][None, :]).astype(BF16)
    key_copy = pltpu.make_async_remote_copy(
        src_ref=key_send.at[:, pl.ds(pl.multiple_of(other * share, share), share)], dst_ref=key_recv,
        send_sem=send_sem.at[blocks], recv_sem=recv_sem.at[blocks],
        device_id={"tensor": other}, device_id_type=pl.DeviceIdType.MESH,
    )
    key_copy.start()

    exchange(q_blocks).wait_recv()
    total = acc[q_blocks] + recv[q_blocks].astype(F32)
    scale = lax.rsqrt(jnp.mean(total * total, axis=1, keepdims=True) + 1e-06)
    kv_lat[...] = (total * scale * kv_gain[...][None, :]).astype(BF16)
    key_copy.wait_recv()
    key_sum[...] = key_acc[:, pl.ds(pl.multiple_of(me * share, share), share)] + key_recv[...].astype(F32)
    for n in range(blocks):
        exchange(n).wait_send()
    key_copy.wait_send()


def down(hidden, w_dq, w_dkv, q_gain, kv_gain):
    rows, depth = hidden.shape
    q_width = w_dq.shape[1]
    width = kv_gain.shape[0]
    rope_width = w_dkv.shape[1] - width
    q_blocks = q_width // width
    blocks = q_blocks + 1
    share = rows // lax.axis_size("tensor")
    vmem = pl.BlockSpec(memory_space=pltpu.VMEM)
    hbm = pl.BlockSpec(memory_space=pl.ANY)
    return pl.pallas_call(
        down_kernel,
        out_shape=(
            jax.ShapeDtypeStruct((rows, q_width), BF16),
            jax.ShapeDtypeStruct((rows, width), BF16),
            jax.ShapeDtypeStruct((rope_width, share), F32),
        ),
        in_specs=[hbm, hbm, hbm, vmem, vmem],
        out_specs=(vmem, vmem, vmem),
        scratch_shapes=[
            pltpu.VMEM((rows, depth), BF16),
            pltpu.VMEM((q_blocks, depth, width), BF16),
            pltpu.VMEM((width + rope_width, depth), BF16),
            pltpu.VMEM((blocks, rows, width), F32),
            pltpu.VMEM((rope_width, rows), F32),
            pltpu.VMEM((blocks, rows, width), BF16),
            pltpu.VMEM((blocks, rows, width), BF16),
            pltpu.VMEM((rope_width, rows), BF16),
            pltpu.VMEM((rope_width, share), BF16),
            pltpu.SemaphoreType.DMA((CHUNKS,)),
            pltpu.SemaphoreType.DMA((blocks,)),
            pltpu.SemaphoreType.DMA((blocks + 1,)),
            pltpu.SemaphoreType.DMA((blocks + 1,)),
        ],
        compiler_params=pltpu.CompilerParams(
            collective_id=0, has_side_effects=True, vmem_limit_bytes=60 * 1024 * 1024
        ),
        name="down",
    )(hidden, w_dq, w_dkv.T, q_gain, kv_gain)


def up_kernel(q_lat, kv_lat, key_sum, key_tab, tab, w_uq, w_ukv, queries, keys_values, rotary_key, cosine, sine):
    half = ROPE // 2
    lanes = 2 * ROPE
    lane = lax.broadcasted_iota(jnp.int32, (1, lanes), 1)
    first = lane % ROPE < half

    @pl.when(pl.program_id(0) == 0)
    def _():
        both = tab[...]
        cosine[...] = jnp.where(first, both, pltpu.roll(both, half, 1))
        sine[...] = jnp.where(first, -pltpu.roll(both, lanes - half, 1), both)
        one, two = key_sum[:half], key_sum[half:]
        share = key_sum.shape[1]
        own = pl.ds(pl.multiple_of(lax.axis_index("tensor") * share, share), share)
        cos, sin = key_tab[:half, own], key_tab[half:, own]
        rotary_key[:half] = (one * cos - two * sin).astype(BF16)
        rotary_key[half:] = (two * cos + one * sin).astype(BF16)

    full = jnp.dot(q_lat[...], w_uq[...], preferred_element_type=F32)
    low = lane < ROPE
    pair = 2 * (NOPE + ROPE)
    for start in range(0, full.shape[1], pair):
        one = full[:, start + NOPE : start + 2 * NOPE]
        two = full[:, start + 2 * NOPE : start + pair]
        rope = jnp.where(low, one, two)
        swapped = jnp.where(
            first, pltpu.roll(rope, lanes - half, 1), pltpu.roll(rope, half, 1)
        )
        turned = rope * cosine[...] + swapped * sine[...]
        queries[:, start : start + NOPE] = full[:, start : start + NOPE].astype(BF16)
        queries[:, start + NOPE : start + 2 * NOPE] = jnp.where(low, turned, one).astype(BF16)
        queries[:, start + 2 * NOPE : start + pair] = jnp.where(low, two, turned).astype(BF16)
    keys_values[...] = jnp.dot(
        kv_lat[...], w_ukv[...], preferred_element_type=F32
    ).astype(BF16)


def up(q_lat, kv_lat, key_sum, key_tab, tab, w_uq, w_ukv):
    rows, q_width = q_lat.shape
    width = kv_lat.shape[1]
    q_cols = HEADS_PER_STEP * (NOPE + ROPE)
    steps = w_uq.shape[1] // q_cols
    kv_cols = w_ukv.shape[1] // steps
    fixed = lambda *shape: pl.BlockSpec(shape, lambda i: (0, 0))
    moving = lambda *shape: pl.BlockSpec(shape, lambda i: (0, i))
    return pl.pallas_call(
        up_kernel,
        grid=(steps,),
        out_shape=(
            jax.ShapeDtypeStruct((rows, w_uq.shape[1]), BF16),
            jax.ShapeDtypeStruct((rows, w_ukv.shape[1]), BF16),
            jax.ShapeDtypeStruct(key_sum.shape, BF16),
        ),
        in_specs=[
            fixed(rows, q_width),
            fixed(rows, width),
            fixed(*key_sum.shape),
            fixed(*key_tab.shape),
            fixed(*tab.shape),
            moving(q_width, q_cols),
            moving(width, kv_cols),
        ],
        out_specs=(moving(rows, q_cols), moving(rows, kv_cols), fixed(*key_sum.shape)),
        scratch_shapes=[pltpu.VMEM(tab.shape, F32), pltpu.VMEM(tab.shape, F32)],
        compiler_params=pltpu.CompilerParams(
            dimension_semantics=("arbitrary",), vmem_limit_bytes=60 * 1024 * 1024
        ),
        name="up",
    )(q_lat, kv_lat, key_sum, key_tab, tab, w_uq, w_ukv)


def normalize(block, gain):
    scale = lax.rsqrt(jnp.mean(block * block, axis=1, keepdims=True) + 1e-06)
    return (block * scale * gain[None, :]).astype(BF16)


def down_any(hidden, w_dq, w_dkv, q_gain, kv_gain):
    q_width = w_dq.shape[1]
    kv_end = q_width + kv_gain.shape[0]
    partial = jnp.concatenate(
        [
            jnp.dot(hidden, w_dq, preferred_element_type=F32),
            jnp.dot(hidden, w_dkv, preferred_element_type=F32),
        ],
        axis=1,
    )
    own = lax.psum_scatter(partial, "tensor", scatter_dimension=0, tiled=True)
    latent = jnp.concatenate(
        [normalize(own[:, :q_width], q_gain), normalize(own[:, q_width:kv_end], kv_gain)],
        axis=1,
    )
    latent = lax.all_gather(latent, "tensor", axis=0, tiled=True)
    return latent[:, :q_width], latent[:, q_width:], own[:, kv_end:].T


def shards(hidden, w_dq, w_dkv, q_gain, kv_gain, w_uq, w_ukv):
    project = down if lax.axis_size("tensor") == 2 else down_any
    q_lat, kv_lat, key_sum = project(hidden, w_dq, w_dkv, q_gain, kv_gain)
    tab = table(hidden.shape[0], ROPE // 2)
    key_tab = jnp.asarray(tab[:, :ROPE].T)
    queries, keys_values, rotary_key = up(
        q_lat, kv_lat, key_sum, key_tab, jnp.asarray(tab), w_uq, w_ukv
    )
    return queries, keys_values, rotary_key.T


def solution(mesh):
    in_specs = (
        P("dp", "tensor"),
        P("tensor", None),
        P("tensor", None),
        P(),
        P(),
        P(None, "tensor"),
        P(None, "tensor"),
    )
    out_specs = (P("dp", "tensor"), P("dp", "tensor"), P(("dp", "tensor"), None))
    return jax.shard_map(shards, mesh=mesh, in_specs=in_specs, out_specs=out_specs, check_vma=False)
```

```python
import functools

import jax
import jax.numpy as jnp
import numpy as np
from jax import lax
from jax.experimental import pallas as pl
from jax.experimental.pallas import tpu as pltpu
from jax.sharding import PartitionSpec as P

NOPE = 128
ROPE = 64
CHUNKS = 4
HEADS_PER_STEP = 4
F32 = jnp.float32
BF16 = jnp.bfloat16


def table(count, half):
    freqs = np.float32(50000.0) ** (-np.arange(half, dtype=np.float32) / np.float32(half))
    angle = np.arange(count, dtype=np.float32)[:, None] * freqs.astype(np.float32)[None, :]
    angle = angle.astype(np.float64)
    both = np.concatenate([np.cos(angle), np.sin(angle)], axis=1).astype(np.float32)
    return np.concatenate([both, both], axis=1)


def down_kernel(
    hidden_hbm, w_dq_hbm, w_dkv_t_hbm, q_gain, kv_gain,
    q_lat, kv_lat, key_sum,
    hidden, w_q, w_kv, acc, key_acc, send, recv, key_send, key_recv,
    hid_sem, w_sem, send_sem, recv_sem,
):
    me = lax.axis_index("tensor")
    other = 1 - me
    rows = hidden.shape[0]
    width = acc.shape[2]
    q_blocks = w_q.shape[0]
    blocks = q_blocks + 1
    part = rows // CHUNKS
    share = key_recv.shape[1]
    across = (((1,), (1,)), ((), ()))

    def load_hidden(m):
        at = pl.ds(m * part, part)
        return pltpu.make_async_copy(hidden_hbm.at[at], hidden.at[at], hid_sem.at[m])

    def load_w(n):
        if n < q_blocks:
            return pltpu.make_async_copy(
                w_dq_hbm.at[:, pl.ds(n * width, width)], w_q.at[n], w_sem.at[n]
            )
        return pltpu.make_async_copy(w_dkv_t_hbm, w_kv, w_sem.at[n])

    def exchange(n):
        return pltpu.make_async_remote_copy(
            src_ref=send.at[n], dst_ref=recv.at[n],
            send_sem=send_sem.at[n], recv_sem=recv_sem.at[n],
            device_id={"tensor": other}, device_id_type=pl.DeviceIdType.MESH,
        )

    load_hidden(0).start()
    load_w(0).start()
    for m in range(1, CHUNKS):
        load_hidden(m).start()
    for n in range(1, blocks):
        load_w(n).start()

    barrier = pltpu.get_barrier_semaphore()
    pl.semaphore_signal(
        barrier, inc=1, device_id={"tensor": other}, device_id_type=pl.DeviceIdType.MESH
    )
    pl.semaphore_wait(barrier, 1)

    def gather(n):
        total = acc[n] + recv[n].astype(F32)
        acc[n] = total
        return jnp.sum(total * total, axis=1, keepdims=True)

    load_w(0).wait()
    for m in range(CHUNKS):
        load_hidden(m).wait()
        at = pl.ds(m * part, part)
        piece = jnp.dot(hidden[at], w_q[0], preferred_element_type=F32)
        acc[0, at] = piece
        send[0, at] = piece.astype(BF16)
    exchange(0).start()

    squares = None
    for n in range(1, blocks):
        load_w(n).wait()
        if n >= 2:
            exchange(n - 2).wait_recv()
        if n < q_blocks:
            piece = jnp.dot(hidden[...], w_q[n], preferred_element_type=F32)
        else:
            piece = lax.dot_general(
                hidden[...], w_kv[:width], across, preferred_element_type=F32
            )
        acc[n] = piece
        send[n] = piece.astype(BF16)
        if n >= 2:
            more = gather(n - 2)
            squares = more if squares is None else squares + more
        exchange(n).start()

    exchange(q_blocks - 1).wait_recv()
    piece = lax.dot_general(
        w_kv[width:], hidden[...], across, preferred_element_type=F32
    )
    key_acc[...] = piece
    key_send[...] = piece.astype(BF16)
    more = gather(q_blocks - 1)
    squares = more if squares is None else squares + more
    scale = lax.rsqrt(squares / (q_blocks * width) + 1e-06)
    for n in range(q_blocks):
        at = pl.ds(n * width, width)
        q_lat[:, at] = (acc[n] * scale * q_gain[at][None, :]).astype(BF16)
    key_copy = pltpu.make_async_remote_copy(
        src_ref=key_send.at[:, pl.ds(pl.multiple_of(other * share, share), share)], dst_ref=key_recv,
        send_sem=send_sem.at[blocks], recv_sem=recv_sem.at[blocks],
        device_id={"tensor": other}, device_id_type=pl.DeviceIdType.MESH,
    )
    key_copy.start()

    exchange(q_blocks).wait_recv()
    total = acc[q_blocks] + recv[q_blocks].astype(F32)
    scale = lax.rsqrt(jnp.mean(total * total, axis=1, keepdims=True) + 1e-06)
    kv_lat[...] = (total * scale * kv_gain[...][None, :]).astype(BF16)
    key_copy.wait_recv()
    key_sum[...] = key_acc[:, pl.ds(pl.multiple_of(me * share, share), share)] + key_recv[...].astype(F32)
    for n in range(blocks):
        exchange(n).wait_send()
    key_copy.wait_send()


def down(hidden, w_dq, w_dkv, q_gain, kv_gain):
    rows, depth = hidden.shape
    q_width = w_dq.shape[1]
    width = kv_gain.shape[0]
    rope_width = w_dkv.shape[1] - width
    q_blocks = q_width // width
    blocks = q_blocks + 1
    share = rows // lax.axis_size("tensor")
    vmem = pl.BlockSpec(memory_space=pltpu.VMEM)
    hbm = pl.BlockSpec(memory_space=pl.ANY)
    return pl.pallas_call(
        down_kernel,
        out_shape=(
            jax.ShapeDtypeStruct((rows, q_width), BF16),
            jax.ShapeDtypeStruct((rows, width), BF16),
            jax.ShapeDtypeStruct((rope_width, share), F32),
        ),
        in_specs=[hbm, hbm, hbm, vmem, vmem],
        out_specs=(vmem, vmem, vmem),
        scratch_shapes=[
            pltpu.VMEM((rows, depth), BF16),
            pltpu.VMEM((q_blocks, depth, width), BF16),
            pltpu.VMEM((width + rope_width, depth), BF16),
            pltpu.VMEM((blocks, rows, width), F32),
            pltpu.VMEM((rope_width, rows), F32),
            pltpu.VMEM((blocks, rows, width), BF16),
            pltpu.VMEM((blocks, rows, width), BF16),
            pltpu.VMEM((rope_width, rows), BF16),
            pltpu.VMEM((rope_width, share), BF16),
            pltpu.SemaphoreType.DMA((CHUNKS,)),
            pltpu.SemaphoreType.DMA((blocks,)),
            pltpu.SemaphoreType.DMA((blocks + 1,)),
            pltpu.SemaphoreType.DMA((blocks + 1,)),
        ],
        compiler_params=pltpu.CompilerParams(
            collective_id=0, has_side_effects=True, vmem_limit_bytes=47 * 1024 * 1024
        ),
        name="down",
    )(hidden, w_dq, w_dkv.T, q_gain, kv_gain)


def up_kernel(q_lat, kv_lat, key_sum, key_tab, tab, w_uq, w_ukv, queries, keys_values, rotary_key, cosine, sine):
    half = ROPE // 2
    lanes = 2 * ROPE
    lane = lax.broadcasted_iota(jnp.int32, (1, lanes), 1)
    first = lane % ROPE < half

    @pl.when(pl.program_id(0) == 0)
    def _():
        both = tab[...]
        cosine[...] = jnp.where(first, both, pltpu.roll(both, half, 1))
        sine[...] = jnp.where(first, -pltpu.roll(both, lanes - half, 1), both)
        one, two = key_sum[:half], key_sum[half:]
        share = key_sum.shape[1]
        own = pl.ds(pl.multiple_of(lax.axis_index("tensor") * share, share), share)
        cos, sin = key_tab[:half, own], key_tab[half:, own]
        rotary_key[:half] = (one * cos - two * sin).astype(BF16)
        rotary_key[half:] = (two * cos + one * sin).astype(BF16)

    full = jnp.dot(q_lat[...], w_uq[...], preferred_element_type=F32)
    low = lane < ROPE
    pair = 2 * (NOPE + ROPE)
    for start in range(0, full.shape[1], pair):
        one = full[:, start + NOPE : start + 2 * NOPE]
        two = full[:, start + 2 * NOPE : start + pair]
        rope = jnp.where(low, one, two)
        swapped = jnp.where(
            first, pltpu.roll(rope, lanes - half, 1), pltpu.roll(rope, half, 1)
        )
        turned = rope * cosine[...] + swapped * sine[...]
        queries[:, start : start + NOPE] = full[:, start : start + NOPE].astype(BF16)
        queries[:, start + NOPE : start + 2 * NOPE] = jnp.where(low, turned, one).astype(BF16)
        queries[:, start + 2 * NOPE : start + pair] = jnp.where(low, two, turned).astype(BF16)
    keys_values[...] = jnp.dot(
        kv_lat[...], w_ukv[...], preferred_element_type=F32
    ).astype(BF16)


def up(q_lat, kv_lat, key_sum, key_tab, tab, w_uq, w_ukv):
    rows, q_width = q_lat.shape
    width = kv_lat.shape[1]
    q_cols = HEADS_PER_STEP * (NOPE + ROPE)
    steps = w_uq.shape[1] // q_cols
    kv_cols = w_ukv.shape[1] // steps
    fixed = lambda *shape: pl.BlockSpec(shape, lambda i: (0, 0))
    moving = lambda *shape: pl.BlockSpec(shape, lambda i: (0, i))
    return pl.pallas_call(
        up_kernel,
        grid=(steps,),
        out_shape=(
            jax.ShapeDtypeStruct((rows, w_uq.shape[1]), BF16),
            jax.ShapeDtypeStruct((rows, w_ukv.shape[1]), BF16),
            jax.ShapeDtypeStruct(key_sum.shape, BF16),
        ),
        in_specs=[
            fixed(rows, q_width),
            fixed(rows, width),
            fixed(*key_sum.shape),
            fixed(*key_tab.shape),
            fixed(*tab.shape),
            moving(q_width, q_cols),
            moving(width, kv_cols),
        ],
        out_specs=(moving(rows, q_cols), moving(rows, kv_cols), fixed(*key_sum.shape)),
        scratch_shapes=[pltpu.VMEM(tab.shape, F32), pltpu.VMEM(tab.shape, F32)],
        compiler_params=pltpu.CompilerParams(
            dimension_semantics=("arbitrary",), vmem_limit_bytes=40 * 1024 * 1024
        ),
        name="up",
    )(q_lat, kv_lat, key_sum, key_tab, tab, w_uq, w_ukv)


def normalize(block, gain):
    scale = lax.rsqrt(jnp.mean(block * block, axis=1, keepdims=True) + 1e-06)
    return (block * scale * gain[None, :]).astype(BF16)


def down_any(hidden, w_dq, w_dkv, q_gain, kv_gain):
    q_width = w_dq.shape[1]
    kv_end = q_width + kv_gain.shape[0]
    partial = jnp.concatenate(
        [
            jnp.dot(hidden, w_dq, preferred_element_type=F32),
            jnp.dot(hidden, w_dkv, preferred_element_type=F32),
        ],
        axis=1,
    )
    own = lax.psum_scatter(partial, "tensor", scatter_dimension=0, tiled=True)
    latent = jnp.concatenate(
        [normalize(own[:, :q_width], q_gain), normalize(own[:, q_width:kv_end], kv_gain)],
        axis=1,
    )
    latent = lax.all_gather(latent, "tensor", axis=0, tiled=True)
    return latent[:, :q_width], latent[:, q_width:], own[:, kv_end:].T


def shards(hidden, w_dq, w_dkv, q_gain, kv_gain, w_uq, w_ukv):
    project = down if lax.axis_size("tensor") == 2 else down_any
    q_lat, kv_lat, key_sum = project(hidden, w_dq, w_dkv, q_gain, kv_gain)
    tab = table(hidden.shape[0], ROPE // 2)
    key_tab = jnp.asarray(tab[:, :ROPE].T)
    queries, keys_values, rotary_key = up(
        q_lat, kv_lat, key_sum, key_tab, jnp.asarray(tab), w_uq, w_ukv
    )
    return queries, keys_values, rotary_key.T


def solution(mesh):
    in_specs = (
        P("dp", "tensor"),
        P("tensor", None),
        P("tensor", None),
        P(),
        P(),
        P(None, "tensor"),
        P(None, "tensor"),
    )
    out_specs = (P("dp", "tensor"), P("dp", "tensor"), P(("dp", "tensor"), None))
    return jax.shard_map(shards, mesh=mesh, in_specs=in_specs, out_specs=out_specs, check_vma=False)
```
